32 devices in a mesh: fsdp: 4 (over z), tp: 4 (over y, x), job: 2 (over core).
Axes of the slice: x: 2, y: 2, z: 4, core: 2. Of those that a mesh axis runs over, the one named last changes fastest.
Arguments:
- slopes_in: float32 [128, 128, 1024], P('job', 'fsdp', 'tp'), parts along dimension 0, may hold values from -6 to 6
- moments_in: float32 [128, 128, 1024], P('job', 'fsdp', 'tp'), parts along dimension 0, may hold values from -6 to 6
- weights_in: float32 [128, 128, 1024], P('job', 'fsdp', 'tp'), parts along dimension 0, may hold values from -0.1875 to 0.1875
Outputs:
- new_weights: float32 [128, 128, 1024], P('job', 'fsdp', 'tp'), parts along dimension 0
- new_momentum: float32 [128, 128, 1024], P('job', 'fsdp', 'tp'), parts along dimension 0
The draws below stay inside these ranges and needn't reach their ends.
There are 2 independent parts, one for each index of `job`. The reference program is written for one: setup_inputs(seed, part) draws one part's arguments, and reference() takes and returns one part's arrays. A program takes and returns all parts, laid end to end along the dimension named above; each array names one. Nothing has to cross between parts.
All inputs are finite; a program needn't handle non-finite values.
Results may differ from the reference program's by a relative error of at most 0.00019.
Values sent between devices are 32-bit elements; how exact they have to be, the bound alone decides.
A program may use at most 128 MiB of HBM per device.

```python
import jax
import jax.numpy as jnp
from jax import lax

SIDE = 128
WIDE = 1024
MATS = 64
ITERS = 5


def steps_of(stream_key, dims, shards, smallest, largest):
    def one(dim, parts):
        heights = jax.random.uniform(jax.random.fold_in(jax.random.fold_in(stream_key, 6), dim), (parts,), jnp.float32, smallest / len(shards), largest / len(shards))
        return jnp.repeat(jnp.exp(heights), dims[dim] // parts).reshape((-1,) + (1,) * (len(dims) - dim - 1))

    factor_of = one(*shards[0])
    for cut in shards[1:]:
        factor_of = factor_of * one(*cut)
    return factor_of


def scatter_about(own_key, extent, scale, bound, pieces=(), kind=jnp.bfloat16):
    drawn = jax.random.normal(own_key, extent, jnp.float32) * scale
    if len(pieces) > 0:
        drawn = steps_of(own_key, extent, pieces, -0.22, 0.18) * drawn
    return jnp.clip(drawn, min=-bound, max=bound).astype(kind)


def setup_inputs(seed: int = 0, part: int = 0) -> dict:
    arg_keys = jax.random.split(jax.random.key(seed), 4)
    part_splits = jax.random.split(jax.random.fold_in(arg_keys[3], part), 4)
    return {
        "slopes_in": scatter_about(part_splits[0], (MATS, SIDE, WIDE), 1.0, 6.0, ((1, 4), (2, 4)), jnp.float32),
        "moments_in": scatter_about(part_splits[1], (MATS, SIDE, WIDE), 1.0, 6.0, ((1, 4), (2, 4)), jnp.float32),
        "weights_in": scatter_about(part_splits[2], (MATS, SIDE, WIDE), 0.03, 0.1875, ((1, 4), (2, 4)), jnp.float32),
    }


hold_rate = 0.9
learn_rate = 0.8

def reference(slopes_in, moments_in, weights_in):
    new_momentum = hold_rate * moments_in + slopes_in

    def orthogonal_one(stack):
        iterate = stack[None]
        iterate = iterate * lax.rsqrt(lax.optimization_barrier(jnp.sum(iterate * iterate, axis=(1, 2), keepdims=True)) + 1e-06)
        for step in range(ITERS):
            gram = jnp.einsum('mik,mjk->mij', iterate, iterate, precision=lax.Precision.HIGHEST)
            mixed = -4.775 * gram + 2.0315 * jnp.einsum('mij,mjk->mik', gram, gram, precision=lax.Precision.HIGHEST)
            iterate = 3.4445 * iterate + jnp.einsum('mij,mjk->mik', mixed, iterate, precision=lax.Precision.HIGHEST)
        return iterate[0]
    iterate = lax.map(orthogonal_one, new_momentum)
    new_weights = weights_in - learn_rate * iterate
    return (new_weights, new_momentum)
```

```python
import functools

import jax
import jax.numpy as jnp
from jax import lax
from jax.experimental import pallas as pl
from jax.experimental.pallas import tpu as pltpu
from jax.sharding import PartitionSpec as P

ITERS = 5


hold_rate = 0.9
learn_rate = 0.8

COEF_A, COEF_B, COEF_C = 3.4445, -4.775, 2.0315
MESH = pl.DeviceIdType.MESH
HIGHEST = lax.Precision.HIGHEST


def dot(a, b, contract=((1,), (0,))):
    return lax.dot_general(
        a, b, (contract, ((), ())), precision=HIGHEST, preferred_element_type=jnp.float32
    )


def factor_of(gram):
    side = gram.shape[0]
    rows = lax.broadcasted_iota(jnp.int32, (side, side), 0)
    eye = rows == lax.broadcasted_iota(jnp.int32, (side, side), 1)
    total = jnp.sum(jnp.where(eye, gram, 0.0), axis=(0, 1), keepdims=True)
    scale = lax.rsqrt(total + 1e-06)

    def mixed_of(a):
        return COEF_B * a + COEF_C * dot(a, a)

    def step(_, carry):
        a, q = carry
        mixed = mixed_of(a)
        half = COEF_A * a + dot(mixed, a)
        return COEF_A * half + dot(half, mixed), COEF_A * q + dot(mixed, q)

    a = gram * scale * scale
    q = jnp.where(eye, jnp.broadcast_to(scale, gram.shape), 0.0)
    a, q = lax.fori_loop(0, ITERS - 1, step, (a, q))
    return COEF_A * q + dot(mixed_of(a), q)


def kernel(nf, nt, chunks, mom, out, xbuf, gsend, grecv, qrecv, ybuf, fsend, frecv, gs, gr, qs, qr, bsend, brecv, own):
    me_f, me_t = lax.axis_index("fsdp"), lax.axis_index("tp")
    mats, rows, _ = mom.shape
    share = mats // nf
    per = share // chunks
    each = per // nt

    barrier = pltpu.get_barrier_semaphore()
    for d in range(1, nf):
        pl.semaphore_signal(barrier, inc=1, device_id={"fsdp": lax.rem(me_f + d, nf)}, device_id_type=MESH)
    for d in range(1, nt):
        pl.semaphore_signal(barrier, inc=1, device_id={"tp": lax.rem(me_t + d, nt)}, device_id_type=MESH)
    pl.semaphore_wait(barrier, nf + nt - 2)

    my_rows = pl.ds(pl.multiple_of(me_f * rows, rows), rows)

    def there(c, d):
        peer = lax.rem(me_f + d, nf)
        return pltpu.make_async_remote_copy(
            src_ref=mom.at[pl.ds(peer * share + c * per, per)],
            dst_ref=xbuf.at[pl.ds(c * per, per), my_rows, :],
            send_sem=fsend.at[c, d - 1], recv_sem=frecv.at[c, d - 1],
            device_id={"fsdp": peer}, device_id_type=MESH,
        )

    def stay(c):
        return pltpu.make_async_copy(
            mom.at[pl.ds(me_f * share + c * per, per)],
            xbuf.at[pl.ds(c * per, per), my_rows, :], own.at[0, c],
        )

    def back(c, d):
        peer = lax.rem(me_f + d, nf)
        theirs = pl.ds(pl.multiple_of(peer * rows, rows), rows)
        return pltpu.make_async_remote_copy(
            src_ref=ybuf.at[pl.ds(c * per, per), theirs, :],
            dst_ref=out.at[pl.ds(me_f * share + c * per, per)],
            send_sem=bsend.at[c, d - 1], recv_sem=brecv.at[c, d - 1],
            device_id={"fsdp": peer}, device_id_type=MESH,
        )

    def keep(c):
        return pltpu.make_async_copy(
            ybuf.at[pl.ds(c * per, per), my_rows, :],
            out.at[pl.ds(me_f * share + c * per, per)], own.at[1, c],
        )

    def gram_copy(c, d):
        return pltpu.make_async_remote_copy(
            src_ref=gsend.at[c, d - 1], dst_ref=grecv.at[c, d],
            send_sem=gs.at[c, d - 1], recv_sem=gr.at[c, d - 1],
            device_id={"tp": lax.rem(me_t + d, nt)}, device_id_type=MESH,
        )

    def factor_copy(c, d):
        return pltpu.make_async_remote_copy(
            src_ref=qrecv.at[c, 0], dst_ref=qrecv.at[c, d],
            send_sem=qs.at[c, d - 1], recv_sem=qr.at[c, d - 1],
            device_id={"tp": lax.rem(me_t + d, nt)}, device_id_type=MESH,
        )

    def grams(c):
        stay(c).wait()
        for d in range(1, nf):
            there(c, d).wait_recv()
        for d in list(range(1, nt)) + [0]:
            first = c * per + lax.rem(me_t + d, nt) * each
            for e in range(each):
                x = xbuf[first + e]
                g = dot(x, x, ((1,), (1,)))
                if d == 0:
                    grecv[c, 0, e] = g
                else:
                    gsend[c, d - 1, e] = g
            if d > 0:
                gram_copy(c, d).start()

    def factors(c):
        for d in range(1, nt):
            gram_copy(c, d).wait_recv()
        for e in range(each):
            g = grecv[c, 0, e]
            for d in range(1, nt):
                g = g + grecv[c, d, e]
            qrecv[c, 0, e] = factor_of(g)
        for d in range(1, nt):
            factor_copy(c, d).start()

    def apply(c):
        for d in range(nt):
            if d > 0:
                factor_copy(c, d).wait_recv()
            first = c * per + lax.rem(me_t - d + nt, nt) * each
            for e in range(each):
                ybuf[first + e] = dot(qrecv[c, d, e], xbuf[first + e])
        for d in range(1, nf):
            back(c, d).start()
        keep(c).start()

    for c in range(chunks):
        for d in range(1, nf):
            there(c, d).start()
        stay(c).start()

    for c in range(chunks + 1):
        if c < chunks:
            grams(c)
        if c > 0:
            apply(c - 1)
        if c < chunks:
            factors(c)

    for c in range(chunks):
        keep(c).wait()
        for d in range(1, nf):
            there(c, d).wait_send()
            back(c, d).wait_send()
            back(c, d).wait_recv()
        for d in range(1, nt):
            gram_copy(c, d).wait_send()
            factor_copy(c, d).wait_send()


def orthogonal(nf, nt, new_momentum):
    mats, rows, wide = new_momentum.shape
    side, share = rows * nf, mats // nf
    most = share // nt
    chunks = max(k for k in range(1, 5) if most % k == 0)
    per = share // chunks
    each = per // nt
    vmem, dma = pltpu.VMEM, pltpu.SemaphoreType.DMA
    return pl.pallas_call(
        functools.partial(kernel, nf, nt, chunks),
        out_shape=jax.ShapeDtypeStruct(new_momentum.shape, jnp.float32),
        in_specs=[pl.BlockSpec(memory_space=pltpu.VMEM)],
        out_specs=pl.BlockSpec(memory_space=pltpu.VMEM),
        scratch_shapes=[
            vmem((share, side, wide), jnp.float32),
            vmem((chunks, nt - 1, each, side, side), jnp.float32),
            vmem((chunks, nt, each, side, side), jnp.float32),
            vmem((chunks, nt, each, side, side), jnp.float32),
            vmem((share, side, wide), jnp.float32),
            dma((chunks, nf - 1)), dma((chunks, nf - 1)),
            dma((chunks, nt - 1)), dma((chunks, nt - 1)),
            dma((chunks, nt - 1)), dma((chunks, nt - 1)),
            dma((chunks, nf - 1)), dma((chunks, nf - 1)),
            dma((2, chunks)),
        ],
        compiler_params=pltpu.CompilerParams(
            collective_id=0, has_side_effects=True, vmem_limit_bytes=32 * 2**20
        ),
    )(new_momentum)


def orthogonal_plain(new_momentum):
    moved = lax.all_to_all(new_momentum, "fsdp", split_axis=0, concat_axis=1, tiled=True)
    gram = lax.dot_general(moved, moved, (((2,), (2,)), ((0,), (0,))), precision=HIGHEST)
    gram = lax.psum_scatter(gram, "tp", scatter_dimension=0, tiled=True)
    factors = lax.all_gather(jax.vmap(factor_of)(gram), "tp", axis=0, tiled=True)
    whole = lax.dot_general(factors, moved, (((2,), (1,)), ((0,), (0,))), precision=HIGHEST)
    return lax.all_to_all(whole, "fsdp", split_axis=1, concat_axis=0, tiled=True)


def body(nf, nt, slopes_in, moments_in, weights_in):
    new_momentum = hold_rate * moments_in + slopes_in
    rows, wide = new_momentum.shape[1:]
    if rows % 8 == 0 and wide % 128 == 0:
        iterate = orthogonal(nf, nt, new_momentum)
    else:
        iterate = orthogonal_plain(new_momentum)
    new_weights = weights_in - learn_rate * iterate
    return (new_weights, new_momentum)


def solution(mesh):
    placed = (P("job", "fsdp", "tp"), P("job", "fsdp", "tp"), P("job", "fsdp", "tp"))
    return jax.shard_map(
        functools.partial(body, mesh.shape["fsdp"], mesh.shape["tp"]),
        mesh=mesh,
        in_specs=placed,
        out_specs=(P("job", "fsdp", "tp"), P("job", "fsdp", "tp")),
        check_vma=False,
    )
```

```python
import functools

import jax
import jax.numpy as jnp
from jax import lax
from jax.experimental import pallas as pl
from jax.experimental.pallas import tpu as pltpu
from jax.sharding import PartitionSpec as P

ITERS = 5


hold_rate = 0.9
learn_rate = 0.8

COEF_A, COEF_B, COEF_C = 3.4445, -4.775, 2.0315
MESH = pl.DeviceIdType.MESH
HIGHEST = lax.Precision.HIGHEST


def dot(a, b, contract=((1,), (0,))):
    return lax.dot_general(
        a, b, (contract, ((), ())), precision=HIGHEST, preferred_element_type=jnp.float32
    )


def factor_of(gram):
    side = gram.shape[0]
    rows = lax.broadcasted_iota(jnp.int32, (side, side), 0)
    eye = rows == lax.broadcasted_iota(jnp.int32, (side, side), 1)
    total = jnp.sum(jnp.where(eye, gram, 0.0), axis=(0, 1), keepdims=True)
    scale = lax.rsqrt(total + 1e-06)

    def mixed_of(a):
        return COEF_B * a + COEF_C * dot(a, a)

    def step(_, carry):
        a, q = carry
        mixed = mixed_of(a)
        half = COEF_A * a + dot(mixed, a)
        return COEF_A * half + dot(half, mixed), COEF_A * q + dot(mixed, q)

    a = gram * scale * scale
    q = jnp.where(eye, jnp.broadcast_to(scale, gram.shape), 0.0)
    a, q = lax.fori_loop(0, ITERS - 1, step, (a, q))
    return COEF_A * q + dot(mixed_of(a), q)


def kernel(nf, nt, chunks, slopes, moments, weights, new, mom, out, wbuf, sbuf, mbuf, xbuf, gsend, grecv, qrecv, ybuf, fsend, frecv, gs, gr, qs, qr, bsend, brecv, own, loads):
    me_f, me_t = lax.axis_index("fsdp"), lax.axis_index("tp")
    mats, rows, _ = mom.shape
    share = mats // nf
    per = share // chunks
    each = per // nt

    barrier = pltpu.get_barrier_semaphore()
    for d in range(1, nf):
        pl.semaphore_signal(barrier, inc=1, device_id={"fsdp": lax.rem(me_f + d, nf)}, device_id_type=MESH)
    for d in range(1, nt):
        pl.semaphore_signal(barrier, inc=1, device_id={"tp": lax.rem(me_t + d, nt)}, device_id_type=MESH)

    order = [(c, d) for c in range(chunks) for d in list(range(1, nf)) + [0]]

    def block(c, d):
        return pl.ds(lax.rem(me_f + d, nf) * share + c * per, per)

    def load(c, d):
        here = block(c, d)
        return (
            pltpu.make_async_copy(slopes.at[here], sbuf.at[here], loads.at[0, c, d]),
            pltpu.make_async_copy(moments.at[here], mbuf.at[here], loads.at[1, c, d]),
        )

    for c, d in order:
        for copy in load(c, d):
            copy.start()
    fetch = pltpu.make_async_copy(weights, wbuf, own.at[2, 0])
    fetch.start()

    my_rows = pl.ds(pl.multiple_of(me_f * rows, rows), rows)

    def there(c, d):
        peer = lax.rem(me_f + d, nf)
        return pltpu.make_async_remote_copy(
            src_ref=mom.at[pl.ds(peer * share + c * per, per)],
            dst_ref=xbuf.at[pl.ds(c * per, per), my_rows, :],
            send_sem=fsend.at[c, d - 1], recv_sem=frecv.at[c, d - 1],
            device_id={"fsdp": peer}, device_id_type=MESH,
        )

    def stay(c):
        return pltpu.make_async_copy(
            mom.at[pl.ds(me_f * share + c * per, per)],
            xbuf.at[pl.ds(c * per, per), my_rows, :], own.at[0, c],
        )

    def back(c, d):
        peer = lax.rem(me_f + d, nf)
        theirs = pl.ds(pl.multiple_of(peer * rows, rows), rows)
        return pltpu.make_async_remote_copy(
            src_ref=ybuf.at[pl.ds(c * per, per), theirs, :],
            dst_ref=out.at[pl.ds(me_f * share + c * per, per)],
            send_sem=bsend.at[c, d - 1], recv_sem=brecv.at[c, d - 1],
            device_id={"fsdp": peer}, device_id_type=MESH,
        )

    def keep(c):
        return pltpu.make_async_copy(
            ybuf.at[pl.ds(c * per, per), my_rows, :],
            out.at[pl.ds(me_f * share + c * per, per)], own.at[1, c],
        )

    def gram_copy(c, d):
        return pltpu.make_async_remote_copy(
            src_ref=gsend.at[c, d - 1], dst_ref=grecv.at[c, d],
            send_sem=gs.at[c, d - 1], recv_sem=gr.at[c, d - 1],
            device_id={"tp": lax.rem(me_t + d, nt)}, device_id_type=MESH,
        )

    def factor_copy(c, d):
        return pltpu.make_async_remote_copy(
            src_ref=qrecv.at[c, 0], dst_ref=qrecv.at[c, d],
            send_sem=qs.at[c, d - 1], recv_sem=qr.at[c, d - 1],
            device_id={"tp": lax.rem(me_t + d, nt)}, device_id_type=MESH,
        )

    def grams(c):
        stay(c).wait()
        for d in range(1, nf):
            there(c, d).wait_recv()
        for d in list(range(1, nt)) + [0]:
            first = c * per + lax.rem(me_t + d, nt) * each
            for e in range(each):
                x = xbuf[first + e]
                g = dot(x, x, ((1,), (1,)))
                if d == 0:
                    grecv[c, 0, e] = g
                else:
                    gsend[c, d - 1, e] = g
            if d > 0:
                gram_copy(c, d).start()

    def factors(c):
        for d in range(1, nt):
            gram_copy(c, d).wait_recv()
        for e in range(each):
            g = grecv[c, 0, e]
            for d in range(1, nt):
                g = g + grecv[c, d, e]
            qrecv[c, 0, e] = factor_of(g)
        for d in range(1, nt):
            factor_copy(c, d).start()

    def apply(c):
        for d in range(nt):
            if d > 0:
                factor_copy(c, d).wait_recv()
            first = c * per + lax.rem(me_t - d + nt, nt) * each
            for e in range(each):
                ybuf[first + e] = dot(qrecv[c, d, e], xbuf[first + e])
        for d in range(1, nf):
            back(c, d).start()
        keep(c).start()

    def send(c, d):
        if d > 0:
            there(c, d).start()
        else:
            stay(c).start()

    def momentum(c, d):
        for copy in load(c, d):
            copy.wait()
        here = block(c, d)
        mom[here] = hold_rate * mbuf[here] + sbuf[here]

    for k, (c, d) in enumerate(order):
        momentum(c, d)
        if k == 0:
            pl.semaphore_wait(barrier, nf + nt - 2)
        else:
            send(*order[k - 1])
    send(*order[-1])

    for c in range(chunks + 1):
        if c < chunks:
            grams(c)
        if c > 0:
            apply(c - 1)
        if c < chunks:
            factors(c)

    fetch.wait()
    for c in range(chunks):
        for d in range(nf):
            if d > 0:
                back(c, d).wait_recv()
            else:
                keep(c).wait()
            here = pl.ds(lax.rem(me_f - d + nf, nf) * share + c * per, per)
            new[here] = wbuf[here] - learn_rate * out[here]

    for c in range(chunks):
        for d in range(1, nf):
            there(c, d).wait_send()
            back(c, d).wait_send()
        for d in range(1, nt):
            gram_copy(c, d).wait_send()
            factor_copy(c, d).wait_send()


def finish(new, mom, new_out, mom_out, sems):
    copies = []
    for k, (src, dst) in enumerate(((mom, mom_out), (new, new_out))):
        copies.append(pltpu.make_async_copy(src, dst, sems.at[k]))
    for copy in copies:
        copy.start()
    for copy in copies:
        copy.wait()


def stepped(nf, nt, slopes_in, moments_in, weights_in):
    mats, rows, wide = slopes_in.shape
    side, share = rows * nf, mats // nf
    most = share // nt
    chunks = max(k for k in range(1, 5) if most % k == 0)
    per = share // chunks
    each = per // nt
    vmem, dma = pltpu.VMEM, pltpu.SemaphoreType.DMA
    shape = jax.ShapeDtypeStruct(slopes_in.shape, jnp.float32)
    held = [pl.BlockSpec(memory_space=pltpu.VMEM)] * 2
    far = [pl.BlockSpec(memory_space=pltpu.HBM)]
    results = pl.pallas_call(
        functools.partial(kernel, nf, nt, chunks),
        out_shape=[shape] * 2,
        in_specs=far * 3,
        out_specs=held,
        scratch_shapes=[
            vmem(slopes_in.shape, jnp.float32),
            vmem(slopes_in.shape, jnp.float32),
            vmem(slopes_in.shape, jnp.float32),
            vmem(slopes_in.shape, jnp.float32),
            vmem((share, side, wide), jnp.float32),
            vmem((chunks, nt - 1, each, side, side), jnp.float32),
            vmem((chunks, nt, each, side, side), jnp.float32),
            vmem((chunks, nt, each, side, side), jnp.float32),
            vmem((share, side, wide), jnp.float32),
            dma((chunks, nf - 1)), dma((chunks, nf - 1)),
            dma((chunks, nt - 1)), dma((chunks, nt - 1)),
            dma((chunks, nt - 1)), dma((chunks, nt - 1)),
            dma((chunks, nf - 1)), dma((chunks, nf - 1)),
            dma((3, chunks)), dma((2, chunks, nf)),
        ],
        compiler_params=pltpu.CompilerParams(
            collective_id=0, has_side_effects=True, vmem_limit_bytes=32 * 2**20
        ),
    )(*(pltpu.with_memory_space_constraint(x, pltpu.HBM) for x in (slopes_in, moments_in, weights_in)))
    return pl.pallas_call(
        finish,
        out_shape=[shape] * 2,
        in_specs=held,
        out_specs=far * 2,
        scratch_shapes=[dma((2,))],
        compiler_params=pltpu.CompilerParams(vmem_limit_bytes=2**20),
    )(*results)


def orthogonal_plain(new_momentum):
    moved = lax.all_to_all(new_momentum, "fsdp", split_axis=0, concat_axis=1, tiled=True)
    gram = lax.dot_general(moved, moved, (((2,), (2,)), ((0,), (0,))), precision=HIGHEST)
    gram = lax.psum_scatter(gram, "tp", scatter_dimension=0, tiled=True)
    factors = lax.all_gather(jax.vmap(factor_of)(gram), "tp", axis=0, tiled=True)
    whole = lax.dot_general(factors, moved, (((2,), (1,)), ((0,), (0,))), precision=HIGHEST)
    return lax.all_to_all(whole, "fsdp", split_axis=1, concat_axis=0, tiled=True)


def body(nf, nt, slopes_in, moments_in, weights_in):
    rows, wide = slopes_in.shape[1:]
    if rows % 8 == 0 and wide % 128 == 0:
        return stepped(nf, nt, slopes_in, moments_in, weights_in)
    new_momentum = hold_rate * moments_in + slopes_in
    new_weights = weights_in - learn_rate * orthogonal_plain(new_momentum)
    return (new_weights, new_momentum)


def solution(mesh):
    placed = (P("job", "fsdp", "tp"), P("job", "fsdp", "tp"), P("job", "fsdp", "tp"))
    return jax.shard_map(
        functools.partial(body, mesh.shape["fsdp"], mesh.shape["tp"]),
        mesh=mesh,
        in_specs=placed,
        out_specs=(P("job", "fsdp", "tp"), P("job", "fsdp", "tp")),
        check_vma=False,
    )
```

```python
import functools

import jax
import jax.numpy as jnp
from jax import lax
from jax.experimental import pallas as pl
from jax.experimental.pallas import tpu as pltpu
from jax.sharding import PartitionSpec as P

ITERS = 5


hold_rate = 0.9
learn_rate = 0.8

COEF_A, COEF_B, COEF_C = 3.4445, -4.775, 2.0315
MESH = pl.DeviceIdType.MESH
HIGHEST = lax.Precision.HIGHEST


def dot(a, b, contract=((1,), (0,))):
    return lax.dot_general(
        a, b, (contract, ((), ())), precision=HIGHEST, preferred_element_type=jnp.float32
    )


def factor_of(gram):
    side = gram.shape[0]
    rows = lax.broadcasted_iota(jnp.int32, (side, side), 0)
    eye = rows == lax.broadcasted_iota(jnp.int32, (side, side), 1)
    total = jnp.sum(jnp.where(eye, gram, 0.0), axis=(0, 1), keepdims=True)
    scale = lax.rsqrt(total + 1e-06)

    def mixed_of(a):
        return COEF_B * a + COEF_C * dot(a, a)

    def step(_, carry):
        a, q = carry
        mixed = mixed_of(a)
        half = COEF_A * a + dot(mixed, a)
        return COEF_A * half + dot(half, mixed), COEF_A * q + dot(mixed, q)

    a = gram * scale * scale
    q = jnp.where(eye, jnp.broadcast_to(scale, gram.shape), 0.0)
    a, q = lax.fori_loop(0, ITERS - 1, step, (a, q))
    return COEF_A * q + dot(mixed_of(a), q)


def partner(me, d, n):
    if n & (n - 1):
        return lax.rem(me + d, n), lax.rem(me - d + n, n)
    other, bit = 0, 1
    while bit < n:
        mine = lax.rem(lax.div(me, bit), 2)
        other = other + bit * (1 - mine if d & bit else mine)
        bit *= 2
    return other, other


def kernel(nf, nt, chunks, slopes, moments, weights, new, mom, out, wbuf, sbuf, mbuf, xbuf, gsend, grecv, qrecv, ybuf, fsend, frecv, gs, gr, qs, qr, bsend, brecv, own, loads):
    me_f, me_t = lax.axis_index("fsdp"), lax.axis_index("tp")
    mats, rows, _ = mom.shape
    share = mats // nf
    per = share // chunks
    each = per // nt

    barrier = pltpu.get_barrier_semaphore()
    pairs = [partner(me_f, d, nf) for d in range(nf)]
    goal, source = [a for a, _ in pairs], [b for _, b in pairs]
    for d in range(1, nf):
        pl.semaphore_signal(barrier, inc=1, device_id={"fsdp": goal[d]}, device_id_type=MESH)
    for d in range(1, nt):
        pl.semaphore_signal(barrier, inc=1, device_id={"tp": lax.rem(me_t + d, nt)}, device_id_type=MESH)

    order = [(c, d) for c in range(chunks) for d in (range(nf - 1, -1, -1) if c == 0 else range(nf))]

    def block(c, d):
        return pl.ds(goal[d] * share + c * per, per)

    def load(c, d):
        here = block(c, d)
        return (
            pltpu.make_async_copy(slopes.at[here], sbuf.at[here], loads.at[0, c, d]),
            pltpu.make_async_copy(moments.at[here], mbuf.at[here], loads.at[1, c, d]),
        )

    def begin(chunk):
        for c, d in order:
            if c == chunk:
                for copy in load(c, d):
                    copy.start()

    begin(0)
    fetch = pltpu.make_async_copy(weights, wbuf, own.at[2, 0])

    my_rows = pl.ds(pl.multiple_of(me_f * rows, rows), rows)

    def there(c, d):
        peer = goal[d]
        return pltpu.make_async_remote_copy(
            src_ref=mom.at[pl.ds(peer * share + c * per, per)],
            dst_ref=xbuf.at[pl.ds(c * per, per), my_rows, :],
            send_sem=fsend.at[c, d - 1], recv_sem=frecv.at[c, d - 1],
            device_id={"fsdp": peer}, device_id_type=MESH,
        )

    def stay(c):
        return pltpu.make_async_copy(
            mom.at[pl.ds(me_f * share + c * per, per)],
            xbuf.at[pl.ds(c * per, per), my_rows, :], own.at[0, c],
        )

    def back(c, d):
        peer = goal[d]
        theirs = pl.ds(pl.multiple_of(peer * rows, rows), rows)
        return pltpu.make_async_remote_copy(
            src_ref=ybuf.at[pl.ds(c * per, per), theirs, :],
            dst_ref=out.at[pl.ds(me_f * share + c * per, per)],
            send_sem=bsend.at[c, d - 1], recv_sem=brecv.at[c, d - 1],
            device_id={"fsdp": peer}, device_id_type=MESH,
        )

    def keep(c):
        return pltpu.make_async_copy(
            ybuf.at[pl.ds(c * per, per), my_rows, :],
            out.at[pl.ds(me_f * share + c * per, per)], own.at[1, c],
        )

    def gram_copy(c, d):
        return pltpu.make_async_remote_copy(
            src_ref=gsend.at[c, d - 1], dst_ref=grecv.at[c, d],
            send_sem=gs.at[c, d - 1], recv_sem=gr.at[c, d - 1],
            device_id={"tp": lax.rem(me_t + d, nt)}, device_id_type=MESH,
        )

    def factor_copy(c, d):
        return pltpu.make_async_remote_copy(
            src_ref=qrecv.at[c, 0], dst_ref=qrecv.at[c, d],
            send_sem=qs.at[c, d - 1], recv_sem=qr.at[c, d - 1],
            device_id={"tp": lax.rem(me_t + d, nt)}, device_id_type=MESH,
        )

    def grams(c):
        stay(c).wait()
        for d in range(1, nf):
            there(c, d).wait_recv()
        for d in list(range(1, nt)) + [0]:
            first = c * per + lax.rem(me_t + d, nt) * each
            for e in range(each):
                x = xbuf[first + e]
                g = dot(x, x, ((1,), (1,)))
                if d == 0:
                    grecv[c, 0, e] = g
                else:
                    gsend[c, d - 1, e] = g
            if d > 0:
                gram_copy(c, d).start()

    def factors(c):
        for d in range(1, nt):
            gram_copy(c, d).wait_recv()
        for e in range(each):
            g = grecv[c, 0, e]
            for d in range(1, nt):
                g = g + grecv[c, d, e]
            qrecv[c, 0, e] = factor_of(g)
        for d in range(1, nt):
            factor_copy(c, d).start()

    def apply(c):
        for d in range(nt):
            if d > 0:
                factor_copy(c, d).wait_recv()
            first = c * per + lax.rem(me_t - d + nt, nt) * each
            for e in range(each):
                ybuf[first + e] = dot(qrecv[c, d, e], xbuf[first + e])
        for d in range(1, nf):
            back(c, d).start()
        keep(c).start()

    def send(c, d):
        if d > 0:
            there(c, d).start()
        else:
            stay(c).start()

    def momentum(c, d):
        for copy in load(c, d):
            copy.wait()
        here = block(c, d)
        mom[here] = hold_rate * mbuf[here] + sbuf[here]

    for k, (c, d) in enumerate(order):
        momentum(c, d)
        if k == 0:
            pl.semaphore_wait(barrier, nf + nt - 2)
        else:
            send(*order[k - 1])
        if k % nf == nf - 1 and c + 1 < chunks:
            begin(c + 1)
    send(*order[-1])
    fetch.start()

    for c in range(chunks + 1):
        if c < chunks:
            grams(c)
        if c > 0:
            apply(c - 1)
        if c < chunks:
            factors(c)

    fetch.wait()
    for c in range(chunks):
        for d in range(nf):
            if d > 0:
                back(c, d).wait_recv()
            else:
                keep(c).wait()
            here = pl.ds(source[d] * share + c * per, per)
            new[here] = wbuf[here] - learn_rate * out[here]

    for c in range(chunks):
        for d in range(1, nf):
            there(c, d).wait_send()
            back(c, d).wait_send()
        for d in range(1, nt):
            gram_copy(c, d).wait_send()
            factor_copy(c, d).wait_send()


def finish(new, mom, new_out, mom_out, sems):
    copies = []
    for k, (src, dst) in enumerate(((mom, mom_out), (new, new_out))):
        copies.append(pltpu.make_async_copy(src, dst, sems.at[k]))
    for copy in copies:
        copy.start()
    for copy in copies:
        copy.wait()


def stepped(nf, nt, slopes_in, moments_in, weights_in):
    mats, rows, wide = slopes_in.shape
    side, share = rows * nf, mats // nf
    most = share // nt
    chunks = max(k for k in range(1, 5) if most % k == 0)
    per = share // chunks
    each = per // nt
    vmem, dma = pltpu.VMEM, pltpu.SemaphoreType.DMA
    shape = jax.ShapeDtypeStruct(slopes_in.shape, jnp.float32)
    held = [pl.BlockSpec(memory_space=pltpu.VMEM)] * 2
    far = [pl.BlockSpec(memory_space=pltpu.HBM)]
    results = pl.pallas_call(
        functools.partial(kernel, nf, nt, chunks),
        out_shape=[shape] * 2,
        in_specs=far * 3,
        out_specs=held,
        scratch_shapes=[
            vmem(slopes_in.shape, jnp.float32),
            vmem(slopes_in.shape, jnp.float32),
            vmem(slopes_in.shape, jnp.float32),
            vmem(slopes_in.shape, jnp.float32),
            vmem((share, side, wide), jnp.float32),
            vmem((chunks, nt - 1, each, side, side), jnp.float32),
            vmem((chunks, nt, each, side, side), jnp.float32),
            vmem((chunks, nt, each, side, side), jnp.float32),
            vmem((share, side, wide), jnp.float32),
            dma((chunks, nf - 1)), dma((chunks, nf - 1)),
            dma((chunks, nt - 1)), dma((chunks, nt - 1)),
            dma((chunks, nt - 1)), dma((chunks, nt - 1)),
            dma((chunks, nf - 1)), dma((chunks, nf - 1)),
            dma((3, chunks)), dma((2, chunks, nf)),
        ],
        compiler_params=pltpu.CompilerParams(
            collective_id=0, has_side_effects=True, vmem_limit_bytes=32 * 2**20
        ),
    )(*(pltpu.with_memory_space_constraint(x, pltpu.HBM) for x in (slopes_in, moments_in, weights_in)))
    return pl.pallas_call(
        finish,
        out_shape=[shape] * 2,
        in_specs=held,
        out_specs=far * 2,
        scratch_shapes=[dma((2,))],
        compiler_params=pltpu.CompilerParams(vmem_limit_bytes=2**20),
    )(*results)


def orthogonal_plain(new_momentum):
    moved = lax.all_to_all(new_momentum, "fsdp", split_axis=0, concat_axis=1, tiled=True)
    gram = lax.dot_general(moved, moved, (((2,), (2,)), ((0,), (0,))), precision=HIGHEST)
    gram = lax.psum_scatter(gram, "tp", scatter_dimension=0, tiled=True)
    factors = lax.all_gather(jax.vmap(factor_of)(gram), "tp", axis=0, tiled=True)
    whole = lax.dot_general(factors, moved, (((2,), (1,)), ((0,), (0,))), precision=HIGHEST)
    return lax.all_to_all(whole, "fsdp", split_axis=1, concat_axis=0, tiled=True)


def body(nf, nt, slopes_in, moments_in, weights_in):
    rows, wide = slopes_in.shape[1:]
    if rows % 8 == 0 and wide % 128 == 0:
        return stepped(nf, nt, slopes_in, moments_in, weights_in)
    new_momentum = hold_rate * moments_in + slopes_in
    new_weights = weights_in - learn_rate * orthogonal_plain(new_momentum)
    return (new_weights, new_momentum)


def solution(mesh):
    placed = (P("job", "fsdp", "tp"), P("job", "fsdp", "tp"), P("job", "fsdp", "tp"))
    return jax.shard_map(
        functools.partial(body, mesh.shape["fsdp"], mesh.shape["tp"]),
        mesh=mesh,
        in_specs=placed,
        out_specs=(P("job", "fsdp", "tp"), P("job", "fsdp", "tp")),
        check_vma=False,
    )
```
